32 devices in a mesh: rows: 8 (over z, y), sub: 4 (over x, core).
Axes of the slice: x: 2, y: 2, z: 4, core: 2. Of those that a mesh axis runs over, the one named last changes fastest.
Arguments:
- frames: float32 [15, 32768], P(None, ('rows', 'sub')), may hold values from -1 to 1, as said below
- start_vector: float32 [3, 32768], P(None, ('rows', 'sub')), may hold values from -12 to 12
- edge_blocks: float32 [36, 65536], P(None, ('rows', 'sub')), may hold values from -14.4 to 14.4
- edge_source: int32 [32, 2048], P(('rows', 'sub')), may hold values from 0 to 1023
- edge_target: int32 [32, 2048], P(('rows', 'sub')), may hold values from 0 to 1535, as said below
- edge_count: int32 [32], P(('rows', 'sub')), may hold values from 1024 to 2048, as said below
- send_index: int32 [32, 512], P(('rows', 'sub')), may hold values from 0 to 1024, as said below
Outputs:
- new_frames: float32 [15, 32768], P(None, ('rows', 'sub'))
- last_vector: float32 [3, 32768], P(None, ('rows', 'sub'))
- tridiagonal: float32 [2, 4], replicated
The draws below stay inside these ranges and needn't reach their ends.
Inputs may be any that keep to these rules, and one draw needn't show every extreme that they name: `frames`: each pose's block has orthonormal columns to float32 rounding. `edge_target`: below 1024: a pose of the same device. 1024 + u: halo slot u, whose block u // 16 on the providing device is never empty. `edge_count`: some device uses all 2048 slots. `send_index`: row q holds, in blocks of 16, the local poses that device q provides to device p (block p); a block is all poses or all 1024, which marks it empty; a device's block for itself is empty.
All inputs are finite; a program needn't handle non-finite values.
Results may differ from the reference program's by a relative error of at most 0.0003.
Values sent between devices are 32-bit elements; how exact they have to be, the bound alone decides.
A program may use at most 64 MiB of HBM per device.

```python
import math
import jax
import jax.numpy as jnp
from jax import lax

RANK = 5
DIM = 3
LANCZOS = 4
P_DEV = 1024
SHARDS = 32
N_POSE = 32768
E_DEV = 2048
SLOTS = 16
HALO = 512


def graph_tables(key):
    keys = jax.random.split(jax.random.fold_in(key, 5), 7)
    owner = jnp.arange(SHARDS, dtype=jnp.int32)
    active = jax.random.randint(keys[0], (SHARDS, SHARDS), 0, 2)
    forced = (owner[None, :] == (owner[:, None] + 1) % SHARDS) | (owner[None, :] == (owner[:, None] + SHARDS // 2) % SHARDS)
    active = jnp.where(forced, 1, active)
    active = jnp.where(owner[:, None] == owner[None, :], 0, active)
    provided = jax.random.randint(keys[1], (SHARDS, HALO), 0, P_DEV)
    send_index = jnp.where(jnp.repeat(active, SLOTS, axis=1) == 1, provided, P_DEV)
    counts = jax.random.randint(keys[2], (SHARDS,), E_DEV // 2, E_DEV + 1)
    fullest = jax.random.randint(keys[3], (), 0, SHARDS)
    counts = jnp.where(owner == fullest, E_DEV, counts)
    source = jax.random.randint(keys[4], (SHARDS, E_DEV), 0, P_DEV)
    slot_pick = jax.random.randint(keys[5], (SHARDS, E_DEV), 0, HALO)
    local_pick = jax.random.randint(keys[6], (SHARDS, E_DEV), 0, P_DEV)
    usable = jnp.take_along_axis(active.T, slot_pick // SLOTS, axis=1) == 1
    target = jnp.where(usable, P_DEV + slot_pick, local_pick)
    return (send_index, counts, source, target)


def draw_send_index(key, part):
    return graph_tables(key)[0]


def draw_edge_count(key, part):
    return graph_tables(key)[1]


def draw_edge_source(key, part):
    return graph_tables(key)[2]


def draw_edge_target(key, part):
    return graph_tables(key)[3]


def draw_edge_blocks(key, part):
    key_main, key_scale = jax.random.split(jax.random.fold_in(key, 11), 2)
    edge_total = SHARDS * E_DEV
    column = jnp.arange(edge_total, dtype=jnp.int32)
    ramp_scale = 1.0 + 2.0 * (column // E_DEV).astype(jnp.float32) / (SHARDS - 1)
    spread = jnp.exp(jax.random.uniform(key_scale, (1, edge_total), jnp.float32, math.log(0.4), math.log(4.0)))
    base_draw = jax.random.truncated_normal(key_main, -4.0, 4.0, (36, edge_total), jnp.float32)
    return 0.3 * ramp_scale[None, :] * spread * base_draw


def draw_start_vector(key, part):
    key_main = jax.random.fold_in(key, 17)
    column = jnp.arange(N_POSE, dtype=jnp.int32)
    ramp_scale = 1.0 + 2.0 * column.astype(jnp.float32) / (N_POSE - 1)
    base_draw = jax.random.truncated_normal(key_main, -4.0, 4.0, (DIM, N_POSE), jnp.float32)
    return ramp_scale[None, :] * base_draw


def draw_frames(key, part):
    key_main = jax.random.fold_in(key, 13)
    raw_draw = jax.random.normal(key_main, (RANK, DIM, N_POSE), jnp.float32)
    columns = []
    for index in range(DIM):
        vector = raw_draw[:, index, :]
        for earlier in columns:
            vector = vector - jnp.sum(earlier * vector, axis=0)[None, :] * earlier
        vector = vector / jnp.sqrt(jnp.sum(vector * vector, axis=0))[None, :]
        columns.append(vector)
    return jnp.stack(columns, axis=1).reshape(RANK * DIM, N_POSE)


def setup_inputs(seed: int = 0) -> dict:
    key_of = jax.random.split(jax.random.key(seed), 8)
    return {
        "frames": draw_frames(jax.random.fold_in(key_of[7], 71), 0),
        "start_vector": draw_start_vector(jax.random.fold_in(key_of[7], 71), 0),
        "edge_blocks": draw_edge_blocks(jax.random.fold_in(key_of[7], 71), 0),
        "edge_source": draw_edge_source(jax.random.fold_in(key_of[7], 71), 0),
        "edge_target": draw_edge_target(jax.random.fold_in(key_of[7], 71), 0),
        "edge_count": draw_edge_count(jax.random.fold_in(key_of[7], 71), 0),
        "send_index": draw_send_index(jax.random.fold_in(key_of[7], 71), 0),
    }


polar_steps = 8
step_length = 0.3
epsilon = 1e-06

def endpoints(edge_source, edge_target, edge_count, send_index):
    owner = jnp.arange(SHARDS, dtype=jnp.int32)[:, None]
    first_end = owner * P_DEV + edge_source
    slot_index = jnp.maximum(edge_target - P_DEV, 0)
    peer_index = slot_index // SLOTS
    column = owner * SLOTS + slot_index % SLOTS
    remote = peer_index * P_DEV + send_index[peer_index, column]
    second = jnp.where(edge_target < P_DEV, owner * P_DEV + edge_target, remote)
    live_slot = jnp.arange(E_DEV, dtype=jnp.int32)[None, :] < edge_count[:, None]
    return (first_end.reshape(-1), second.reshape(-1), live_slot.reshape(-1))

def symmetric(edge_blocks):
    blocks_six = edge_blocks.reshape(6, 6, -1)
    return 0.5 * (blocks_six + blocks_six.transpose(1, 0, 2))

def block_product(matrix, field_in):
    return lax.optimization_barrier(jnp.sum(matrix[None, :, :, :] * field_in[:, None, :, :], axis=2))

def multiplier(left_field, right_field):
    product = lax.optimization_barrier(jnp.sum(left_field[:, :, None, :] * right_field[:, None, :, :], axis=0))
    return 0.5 * (product + product.transpose(1, 0, 2))

def right_product(field_in, matrix):
    return lax.optimization_barrier(jnp.sum(field_in[:, :, None, :] * matrix[None, :, :, :], axis=1))

def apply_matrix(field_in, coupling, first_end, second, weight):
    values_first = field_in[:, :, first_end]
    values_second = field_in[:, :, second]
    upper_part = block_product(coupling[:3, :3], values_first) + block_product(coupling[:3, 3:], values_second)
    lower_part = block_product(coupling[3:, :3], values_first) + block_product(coupling[3:, 3:], values_second)
    summed = jnp.zeros_like(field_in)
    summed = summed.at[:, :, first_end].add(upper_part * weight)
    return summed.at[:, :, second].add(lower_part * weight)

def retract(frame_now, gradient, length):
    moved = frame_now - length * gradient
    norms = lax.optimization_barrier(jnp.sum(moved * moved, axis=(0, 1)))
    polar_now = moved * jnp.sqrt(DIM / norms)[None, None, :]
    identity = jnp.eye(DIM, dtype=jnp.float32)[:, :, None]
    for iteration in range(polar_steps):
        gram_matrix = lax.optimization_barrier(jnp.sum(polar_now[:, :, None, :] * polar_now[:, None, :, :], axis=0))
        polar_now = right_product(polar_now, 1.5 * identity - 0.5 * gram_matrix)
    return polar_now

def reference(frames, start_vector, edge_blocks, edge_source, edge_target, edge_count, send_index):
    first_end, second, live_slot = endpoints(edge_source, edge_target, edge_count, send_index)
    weight = live_slot.astype(jnp.float32)
    coupling = symmetric(edge_blocks)
    frame_now = frames.reshape(RANK, DIM, N_POSE)
    euclidean = apply_matrix(frame_now, coupling, first_end, second, weight)
    multipliers = multiplier(frame_now, euclidean)
    gradient = 2.0 * (euclidean - right_product(frame_now, multipliers))
    length = step_length * math.sqrt(N_POSE) / jnp.sqrt(jnp.sum(gradient * gradient) + epsilon)
    retracted = retract(frame_now, gradient, length)
    product_new = apply_matrix(retracted, coupling, first_end, second, weight)
    certificate_mult = multiplier(retracted, product_new)
    entries = DIM * N_POSE

    def certify(vector):
        return apply_matrix(vector, coupling, first_end, second, weight) - right_product(vector, certificate_mult)
    start_field = start_vector.reshape(1, DIM, N_POSE)
    krylov_basis = [start_field / jnp.sqrt(jnp.sum(start_field * start_field) / entries + epsilon)]
    alpha_list = []
    beta_list = []
    for iteration in range(LANCZOS):
        image_vec = certify(krylov_basis[-1])
        projected = [jnp.sum(member * image_vec) / entries for member in krylov_basis]
        for member, coefficient in zip(krylov_basis, projected):
            image_vec = image_vec - coefficient * member
        beta_now = jnp.sqrt(jnp.sum(image_vec * image_vec) / entries + epsilon)
        krylov_basis.append(image_vec / beta_now)
        alpha_list.append(projected[-1])
        beta_list.append(beta_now)
    tridiagonal = jnp.stack([jnp.stack(alpha_list), jnp.stack(beta_list)])
    return (retracted.reshape(RANK * DIM, N_POSE), krylov_basis[-1].reshape(DIM, N_POSE), tridiagonal)
```

```python
import functools

import jax
import jax.numpy as jnp
from jax import lax
from jax.experimental import pallas as pl
from jax.experimental.pallas import tpu as pltpu
from jax.sharding import PartitionSpec as P

RANK = 5
DIM = 3
LANCZOS = 4
LANES = 128
CHUNK = 256
EXCHANGES = 5 + 2 * (LANCZOS - 1) + 1

polar_steps = 8
step_length = 0.3
epsilon = 1e-06

F32 = jnp.float32
BF16 = jnp.bfloat16
MESH = pl.DeviceIdType.MESH


def split_three(x):
    high = x.astype(BF16).astype(F32)
    rest = x - high
    middle = rest.astype(BF16).astype(F32)
    low = rest - middle
    parts = [high, middle, low, jnp.zeros((8, x.shape[1]), F32)]
    return jnp.concatenate(parts, axis=0).astype(BF16)


def fold(y, rows):
    return (y[2 * rows:3 * rows] + y[rows:2 * rows]) + y[:rows]


def dot_nn(a, b):
    return lax.dot_general(a, b, (((1,), (0,)), ((), ())), preferred_element_type=F32)


def dot_nt(a, b):
    return lax.dot_general(a, b, (((1,), (1,)), ((), ())), preferred_element_type=F32)


def total(x):
    return jnp.sum(jnp.sum(x, axis=1, keepdims=True), axis=0, keepdims=True)


def column_sum(x):
    return jnp.sum(x, axis=0, keepdims=True)


def multiplier(left, right):
    raw = [[column_sum(left[d] * right[e]) for e in range(DIM)] for d in range(DIM)]
    return [[0.5 * (raw[d][e] + raw[e][d]) for e in range(DIM)] for d in range(DIM)]


def right_product(field, matrix):
    return [sum(field[d] * matrix[d][e] for d in range(DIM)) for e in range(DIM)]


def kernel(
    shards, sub_size,
    frames, start, blocks, source, target, count, send_index,
    new_frames, last_vector, tridiagonal,
    src_hot, dst_hot, send_hot, coupling, near_first, near_second,
    x_split, h_split, up_split, lo_split, stage, result, send, recv,
    send_sem, recv_sem,
):
    poses = frames.shape[1]
    edges = source.shape[1]
    halo = send_index.shape[1]
    slots = halo // shards
    per = LANES // slots
    lane_blocks = halo // LANES
    row_me, sub_me = lax.axis_index("rows"), lax.axis_index("sub")
    me = row_me * sub_size + sub_me
    entries = float(DIM * poses * shards)

    def peer_of(i):
        peer = lax.rem(me + i, shards)
        return peer, (peer // sub_size, lax.rem(peer, sub_size))

    barrier = pltpu.get_barrier_semaphore()

    @pl.loop(1, shards)
    def _(i):
        pl.semaphore_signal(barrier, inc=1, device_id=peer_of(i)[1], device_id_type=MESH)

    def hot(ref, index, rows):
        step = 32
        width = index.shape[1]
        row = lax.broadcasted_iota(jnp.int32, (step, width), 0)

        @pl.loop(0, rows // step)
        def _(r):
            shifted = index - r * step
            ref[pl.ds(pl.multiple_of(r * step, step), step), :] = jnp.where(
                row == shifted, 1.0, 0.0
            ).astype(BF16)

    lane = lax.broadcasted_iota(jnp.int32, (8, LANES), 1)
    group = lane // slots
    sub_row = lax.broadcasted_iota(jnp.int32, (8, LANES), 0)
    scalar_base = DIM * slots

    def scalar_tile(scalars):
        tile = jnp.zeros((8, LANES), F32)
        for k, value in enumerate(scalars):
            tile = jnp.where((lane == scalar_base + k) & (sub_row == 0), value, tile)
        return tile

    def blocks_loop(body):
        lax.fori_loop(0, lane_blocks, lambda b, c: (body(b), c)[1], 0, unroll=lane_blocks <= 4)

    def post(ex, tiles, scalars):
        extra = scalar_tile(scalars)

        def one(b):
            for j in range(per):
                message = extra
                for t in range(tiles):
                    part = stage[b, 8 * t:8 * t + 8, :]
                    shift = ((t - j) * slots) % LANES
                    part = pltpu.roll(part, shift, 1) if shift else part
                    message = jnp.where(group == t, part, message)
                send[ex, b * per + j] = message

        blocks_loop(one)
        recv[ex, me] = send[ex, me]

        @pl.loop(1, shards)
        def _(i):
            peer, where = peer_of(i)
            pltpu.make_async_remote_copy(
                src_ref=send.at[ex, peer],
                dst_ref=recv.at[ex, me],
                send_sem=send_sem.at[ex],
                recv_sem=recv_sem.at[ex],
                device_id=where,
                device_id_type=MESH,
            ).start()

    def arrive(ex):
        whole = recv.at[ex, pl.ds(0, shards - 1)]
        pltpu.make_async_copy(whole, whole, recv_sem.at[ex]).wait()

    def unpack(ex, tiles):
        def one(b):
            for t in range(tiles):
                value = jnp.zeros((8, LANES), F32)
                for j in range(per):
                    shift = ((j - t) * slots) % LANES
                    part = recv[ex, b * per + j]
                    part = pltpu.roll(part, shift, 1) if shift else part
                    value = jnp.where(group == j, part, value)
                stage[b, 8 * t:8 * t + 8, :] = value

        blocks_loop(one)
        rows = 8 * tiles
        return jnp.concatenate([stage[b, :rows, :] for b in range(lane_blocks)], axis=1)

    def arrived_scalars(ex, number):
        tile = jnp.sum(recv[ex], axis=0)
        return [
            total(jnp.where((lane == scalar_base + k) & (sub_row == 0), tile, 0.0))
            for k in range(number)
        ]

    def stage_field(value, rows, c):
        for k in range(CHUNK // LANES):
            stage[c * (CHUNK // LANES) + k, :rows, :] = value[:, k * LANES:(k + 1) * LANES]

    def chunk_of(c):
        return pl.ds(pl.multiple_of(c * CHUNK, CHUNK), CHUNK)

    def product(x, tiles, ex, scalars, before=None):
        rows = 8 * tiles
        used = 3 * rows + 8
        single = tiles == 1
        x_split[:used, :] = split_three(x)

        @pl.loop(0, halo // CHUNK)
        def _(c):
            value = fold(dot_nn(x_split[:used, :], send_hot[:, chunk_of(c)]), rows)
            stage_field(value, rows, c)

        if before is not None:
            pl.semaphore_wait(barrier, shards - 1)
        post(ex, tiles, scalars)
        if before is not None:
            before()

        @pl.loop(0, edges // CHUNK)
        def _(c):
            at = chunk_of(c)
            near_first[:rows, at] = fold(dot_nn(x_split[:used, :], src_hot[:, at]), rows)
            near_second[:rows, at] = fold(dot_nn(x_split[:used, :], dst_hot[:poses, at]), rows)

        arrive(ex)
        h_split[:used, :] = split_three(unpack(ex, tiles))

        @pl.loop(0, edges // CHUNK)
        def _(c):
            at = chunk_of(c)
            first = near_first[:rows, at]
            second = near_second[:rows, at] + fold(
                dot_nn(h_split[:used, :], dst_hot[poses:, at]), rows
            )
            if single:
                ends = [first[d:d + 1] for d in range(DIM)] + [second[d:d + 1] for d in range(DIM)]
                both = sum(coupling[8 * j:8 * j + 8, at] * ends[j] for j in range(6))
                up_split[:used, at] = split_three(both)
            else:
                ends = [first[8 * d:8 * d + 8] for d in range(DIM)] + [
                    second[8 * d:8 * d + 8] for d in range(DIM)
                ]
                both = [
                    sum(coupling[8 * j + i:8 * j + i + 1, at] * ends[j] for j in range(6))
                    for i in range(6)
                ]
                up_split[:used, at] = split_three(jnp.concatenate(both[:3], axis=0))
                lo_split[:used, at] = split_three(jnp.concatenate(both[3:], axis=0))

        upper = up_split
        lower = up_split if single else lo_split

        def lowered(y):
            return pltpu.roll(y, 8 - DIM, 0) if single else y

        @pl.loop(0, halo // CHUNK)
        def _(c):
            at = pl.ds(pl.multiple_of(poses + c * CHUNK, CHUNK), CHUNK)
            stage_field(lowered(fold(dot_nt(lower[:used, :], dst_hot[at, :]), rows)), rows, c)

        post(ex + 1, tiles, [])

        @pl.loop(0, poses // CHUNK)
        def _(c):
            at = chunk_of(c)
            result[:rows, at] = fold(dot_nt(upper[:used, :], src_hot[at, :]), rows) + lowered(
                fold(dot_nt(lower[:used, :], dst_hot[at, :]), rows)
            )

        arrive(ex + 1)
        h_split[:used, :] = split_three(unpack(ex + 1, tiles))

        @pl.loop(0, poses // CHUNK)
        def _(c):
            at = chunk_of(c)
            result[:rows, at] += fold(dot_nt(h_split[:used, :], send_hot[at, :]), rows)

        return result[:rows, :], arrived_scalars(ex, len(scalars))

    def summed(ex, scalars):
        post(ex, 0, scalars)
        arrive(ex)
        return arrived_scalars(ex, len(scalars))

    hot(send_hot, send_index[...], poses)

    frame_now = []
    padding = jnp.zeros((8 - RANK, poses), F32)
    for d in range(DIM):
        rows = [frames[3 * a + d:3 * a + d + 1, :] for a in range(RANK)]
        frame_now.append(jnp.concatenate(rows + [padding], axis=0))
    vector = [start[d:d + 1, :] for d in range(DIM)]
    copy_row = lax.broadcasted_iota(jnp.int32, (8, poses), 0)

    def build():
        hot(src_hot, source[...], poses)
        hot(dst_hot, target[...], poses + halo)
        live = lax.broadcasted_iota(jnp.int32, (1, edges), 1) < count[...]
        weight = jnp.where(live, 0.5, 0.0)
        for j in range(6):
            for i in range(6):
                a, b = 6 * i + j, 6 * j + i
                coupling[8 * j + i:8 * j + i + 1, :] = weight * (
                    blocks[a:a + 1, :] + blocks[b:b + 1, :]
                )
            coupling[8 * j + 6:8 * j + 8, :] = jnp.zeros((2, edges), F32)

    def stacked(parts):
        return jnp.concatenate(parts, axis=0)

    square = sum(total(v * v) for v in vector)
    joint = stacked([jnp.where(copy_row == RANK, vector[d], frame_now[d]) for d in range(DIM)])
    image, (start_square,) = product(joint, DIM, 0, [square], before=build)
    euclidean = [image[8 * d:8 * d + 8] for d in range(DIM)]
    start_scale = 1.0 / jnp.sqrt(start_square / entries + epsilon)
    start_image = [euclidean[d][RANK:RANK + 1] * start_scale for d in range(DIM)]
    krylov = [[v * start_scale for v in vector]]

    projected = right_product(frame_now, multiplier(frame_now, euclidean))
    gradient = [
        jnp.where(copy_row < RANK, 2.0 * (euclidean[d] - projected[d]), 0.0) for d in range(DIM)
    ]
    (square,) = summed(2, [sum(total(g * g) for g in gradient)])
    length = step_length * (float(poses * shards) ** 0.5) / jnp.sqrt(square + epsilon)
    moved = [frame_now[d] - length * gradient[d] for d in range(DIM)]
    norms = column_sum(sum(m * m for m in moved))
    scale = jnp.sqrt(DIM / norms)
    polar = [m * scale for m in moved]
    for _ in range(polar_steps):
        gram = [[None] * DIM for _ in range(DIM)]
        for d in range(DIM):
            for e in range(d, DIM):
                value = -0.5 * column_sum(polar[d] * polar[e])
                gram[d][e] = gram[e][d] = value + 1.5 if d == e else value
        polar = right_product(polar, gram)
    for d in range(DIM):
        for a in range(RANK):
            new_frames[3 * a + d:3 * a + d + 1, :] = polar[d][a:a + 1]

    image, _ = product(stacked(polar), DIM, 3, [])
    certificate = multiplier(polar, [image[8 * d:8 * d + 8] for d in range(DIM)])

    def certify(image_rows, vec):
        back = right_product(vec, certificate)
        return [image_rows[d] - back[d] for d in range(DIM)]

    images = [certify(start_image, krylov[0])]
    alphas, betas = [], []
    for k in range(LANCZOS):
        current = images[-1]
        dots = [
            total(sum(member[d] * current[d] for d in range(DIM))) for member in krylov
        ] + [total(sum(c * c for c in current))]
        ex = 5 + 2 * k
        if k < LANCZOS - 1:
            rows = stacked(current + [jnp.zeros((8 - DIM, poses), F32)])
            image, sums = product(rows, 1, ex, dots)
            following = certify([image[d:d + 1] for d in range(DIM)], current)
        else:
            sums = summed(ex, dots)
        weights = [s / entries for s in sums[:-1]]
        beta = jnp.sqrt(sums[-1] / entries - sum(h * h for h in weights) + epsilon)
        inverse = 1.0 / beta
        krylov.append([
            (current[d] - sum(h * q[d] for h, q in zip(weights, krylov))) * inverse
            for d in range(DIM)
        ])
        if k < LANCZOS - 1:
            images.append([
                (following[d] - sum(h * w[d] for h, w in zip(weights, images))) * inverse
                for d in range(DIM)
            ])
        alphas.append(weights[-1])
        betas.append(beta)
    for d in range(DIM):
        last_vector[d:d + 1, :] = krylov[-1][d]
    column = lax.broadcasted_iota(jnp.int32, (2, LANCZOS), 1)
    line = lax.broadcasted_iota(jnp.int32, (2, LANCZOS), 0)
    table = jnp.zeros((2, LANCZOS), F32)
    for k in range(LANCZOS):
        table = jnp.where(column == k, jnp.where(line == 0, alphas[k], betas[k]), table)
    tridiagonal[...] = table

    for ex in range(EXCHANGES):
        whole = send.at[ex, pl.ds(0, shards - 1)]
        pltpu.make_async_copy(whole, whole, send_sem.at[ex]).wait()


def on_device(shards, sub_size, frames, start, blocks, source, target, count, send_index):
    poses = frames.shape[1]
    edges = source.shape[1]
    halo = send_index.shape[1]
    vmem = pl.BlockSpec(memory_space=pltpu.VMEM)
    split_rows = 3 * 8 * DIM + 8
    return pl.pallas_call(
        functools.partial(kernel, shards, sub_size),
        out_shape=(
            jax.ShapeDtypeStruct((RANK * DIM, poses), F32),
            jax.ShapeDtypeStruct((DIM, poses), F32),
            jax.ShapeDtypeStruct((2, LANCZOS), F32),
        ),
        in_specs=[vmem] * 7,
        out_specs=(vmem, vmem, vmem),
        scratch_shapes=[
            pltpu.VMEM((poses, edges), BF16),
            pltpu.VMEM((poses + halo, edges), BF16),
            pltpu.VMEM((poses, halo), BF16),
            pltpu.VMEM((48, edges), F32),
            pltpu.VMEM((8 * DIM, edges), F32),
            pltpu.VMEM((8 * DIM, edges), F32),
            pltpu.VMEM((split_rows, poses), BF16),
            pltpu.VMEM((split_rows, halo), BF16),
            pltpu.VMEM((split_rows, edges), BF16),
            pltpu.VMEM((split_rows, edges), BF16),
            pltpu.VMEM((halo // LANES, 8 * DIM, LANES), F32),
            pltpu.VMEM((8 * DIM, poses), F32),
            pltpu.VMEM((EXCHANGES, shards, 8, LANES), F32),
            pltpu.VMEM((EXCHANGES, shards, 8, LANES), F32),
            pltpu.SemaphoreType.DMA((EXCHANGES,)),
            pltpu.SemaphoreType.DMA((EXCHANGES,)),
        ],
        compiler_params=pltpu.CompilerParams(
            collective_id=0, has_side_effects=True, vmem_limit_bytes=60 * 1024 * 1024
        ),
    )(frames, start, blocks, source, target, count.reshape(1, 1), send_index)


def solution(mesh):
    shards = mesh.shape["rows"] * mesh.shape["sub"]
    in_specs = (
        P(None, ("rows", "sub")),
        P(None, ("rows", "sub")),
        P(None, ("rows", "sub")),
        P(("rows", "sub"), None),
        P(("rows", "sub"), None),
        P(("rows", "sub")),
        P(("rows", "sub"), None),
    )
    out_specs = (P(None, ("rows", "sub")), P(None, ("rows", "sub")), P())
    return jax.shard_map(
        functools.partial(on_device, shards, mesh.shape["sub"]),
        mesh=mesh,
        in_specs=in_specs,
        out_specs=out_specs,
        check_vma=False,
    )
```

```python
import functools

import jax
import jax.numpy as jnp
from jax import lax
from jax.experimental import pallas as pl
from jax.experimental.pallas import tpu as pltpu
from jax.sharding import PartitionSpec as P

RANK = 5
DIM = 3
LANCZOS = 4
LANES = 128
CHUNK = 1024
ROWS = {0: 1, 1: 4, DIM: 8}
EXCHANGES = 5 + 2 * (LANCZOS - 1) + 1

polar_steps = 8
step_length = 0.3
epsilon = 1e-06

F32 = jnp.float32
BF16 = jnp.bfloat16
F8 = jnp.float8_e4m3fn
MESH = pl.DeviceIdType.MESH


def split_three(x):
    high = x.astype(BF16).astype(F32)
    rest = x - high
    middle = rest.astype(BF16).astype(F32)
    low = rest - middle
    parts = [high, middle, low, jnp.zeros((8, x.shape[1]), F32)]
    return jnp.concatenate(parts, axis=0).astype(BF16)


def fold(y, rows):
    return (y[2 * rows:3 * rows] + y[rows:2 * rows]) + y[:rows]


def dot_nn(a, b):
    return lax.dot_general(a, b, (((1,), (0,)), ((), ())), preferred_element_type=F32)


def dot_nt(a, b):
    return lax.dot_general(a, b, (((1,), (1,)), ((), ())), preferred_element_type=F32)


def total(x):
    return jnp.sum(jnp.sum(x, axis=1, keepdims=True), axis=0, keepdims=True)


def column_sum(x):
    return jnp.sum(x, axis=0, keepdims=True)


def multiplier(left, right):
    raw = [[column_sum(left[d] * right[e]) for e in range(DIM)] for d in range(DIM)]
    return [[0.5 * (raw[d][e] + raw[e][d]) for e in range(DIM)] for d in range(DIM)]


def right_product(field, matrix):
    return [sum(field[d] * matrix[d][e] for d in range(DIM)) for e in range(DIM)]


def kernel(
    shards, sub_size,
    frames, start, blocks, source, target, count, send_index,
    new_frames, last_vector, tridiagonal,
    src_hot, dst_hot, send_hot, coupling, near_first, near_second,
    x_split, h_split, up_split, lo_split, stage, result, send, recv,
    send_sem, recv_sem,
):
    poses = frames.shape[1]
    edges = source.shape[1]
    halo = send_index.shape[1]
    slots = halo // shards
    per = LANES // slots
    lane_blocks = halo // LANES
    row_me, sub_me = lax.axis_index("rows"), lax.axis_index("sub")
    me = row_me * sub_size + sub_me
    entries = float(DIM * poses * shards)

    def peer_of(i):
        peer = lax.rem(me + i, shards)
        return peer, (peer // sub_size, lax.rem(peer, sub_size))

    barrier = pltpu.get_barrier_semaphore()

    @pl.loop(1, shards)
    def _(i):
        pl.semaphore_signal(barrier, inc=1, device_id=peer_of(i)[1], device_id_type=MESH)

    def hot(ref, index, rows):
        step = 32
        width = index.shape[1]
        row = lax.broadcasted_iota(jnp.int32, (step, width), 0)

        @pl.loop(0, rows // step)
        def _(r):
            shifted = index - r * step
            ref[pl.ds(pl.multiple_of(r * step, step), step), :] = jnp.where(
                row == shifted, 1.0, 0.0
            ).astype(F8)

    lane = lax.broadcasted_iota(jnp.int32, (8, LANES), 1)
    group = lane // slots
    sub_row = lax.broadcasted_iota(jnp.int32, (8, LANES), 0)
    scalar_base = DIM * slots

    def scalar_tile(scalars):
        tile = jnp.zeros((8, LANES), F32)
        for k, value in enumerate(scalars):
            tile = jnp.where((lane == scalar_base + k) & (sub_row == 0), value, tile)
        return tile

    def blocks_loop(body):
        lax.fori_loop(0, lane_blocks, lambda b, c: (body(b), c)[1], 0, unroll=lane_blocks <= 4)

    def post(ex, tiles, scalars):
        extra = scalar_tile(scalars)

        def one(b):
            for j in range(per):
                message = extra
                for t in range(tiles):
                    part = stage[b, 8 * t:8 * t + 8, :]
                    shift = ((t - j) * slots) % LANES
                    part = pltpu.roll(part, shift, 1) if shift else part
                    message = jnp.where(group == t, part, message)
                send[ex, b * per + j] = message

        if tiles:
            blocks_loop(one)
            recv[ex, me] = send[ex, me]
        else:
            send[ex, 0] = extra
            recv[ex, me] = extra

        @pl.loop(1, shards)
        def _(i):
            peer, where = peer_of(i)
            pltpu.make_async_remote_copy(
                src_ref=send.at[ex, peer if tiles else 0, pl.ds(0, ROWS[tiles])],
                dst_ref=recv.at[ex, me, pl.ds(0, ROWS[tiles])],
                send_sem=send_sem.at[ex],
                recv_sem=recv_sem.at[ex],
                device_id=where,
                device_id_type=MESH,
            ).start()

    def arrive(ex, tiles):
        whole = recv.at[ex, pl.ds(0, shards - 1), pl.ds(0, ROWS[tiles])]
        pltpu.make_async_copy(whole, whole, recv_sem.at[ex]).wait()

    def unpack(ex, tiles):
        def one(b):
            for t in range(tiles):
                value = jnp.zeros((8, LANES), F32)
                for j in range(per):
                    shift = ((j - t) * slots) % LANES
                    part = recv[ex, b * per + j]
                    part = pltpu.roll(part, shift, 1) if shift else part
                    value = jnp.where(group == j, part, value)
                stage[b, 8 * t:8 * t + 8, :] = value

        blocks_loop(one)
        rows = 8 * tiles
        return jnp.concatenate([stage[b, :rows, :] for b in range(lane_blocks)], axis=1)

    def arrived_scalars(ex, number):
        tile = jnp.sum(recv[ex, :, 0:1, :], axis=0)
        return [
            jnp.sum(jnp.where(lane[:1] == scalar_base + k, tile, 0.0), axis=1, keepdims=True)
            for k in range(number)
        ]

    def stage_field(value, rows, c):
        for k in range(halo_chunk // LANES):
            stage[c * (halo_chunk // LANES) + k, :rows, :] = value[:, k * LANES:(k + 1) * LANES]

    halo_chunk = min(CHUNK, halo)

    def chunk_of(c, size=CHUNK):
        return pl.ds(pl.multiple_of(c * size, size), size)

    def product(x, tiles, ex, scalars, before=None):
        rows = 8 * tiles
        used = 3 * rows + 8
        single = tiles == 1
        x_split[:used, :] = split_three(x)

        @pl.loop(0, halo // halo_chunk)
        def _(c):
            value = fold(dot_nn(x_split[:used, :], send_hot[:, chunk_of(c, halo_chunk)]), rows)
            stage_field(value, rows, c)

        if before is not None:
            pl.semaphore_wait(barrier, shards - 1)
        post(ex, tiles, scalars)
        if before is not None:
            before()

        @pl.loop(0, edges // CHUNK)
        def _(c):
            at = chunk_of(c)
            near_first[:rows, at] = fold(dot_nn(x_split[:used, :], src_hot[:, at]), rows)
            near_second[:rows, at] = fold(dot_nn(x_split[:used, :], dst_hot[:poses, at]), rows)

        arrive(ex, tiles)
        h_split[:used, :] = split_three(unpack(ex, tiles))

        @pl.loop(0, edges // CHUNK)
        def _(c):
            at = chunk_of(c)
            first = near_first[:rows, at]
            second = near_second[:rows, at] + fold(
                dot_nn(h_split[:used, :], dst_hot[poses:, at]), rows
            )
            if single:
                ends = [first[d:d + 1] for d in range(DIM)] + [second[d:d + 1] for d in range(DIM)]
                both = sum(coupling[8 * j:8 * j + 8, at] * ends[j] for j in range(6))
                up_split[:used, at] = split_three(both)
            else:
                ends = [first[8 * d:8 * d + 8] for d in range(DIM)] + [
                    second[8 * d:8 * d + 8] for d in range(DIM)
                ]
                both = [
                    sum(coupling[8 * j + i:8 * j + i + 1, at] * ends[j] for j in range(6))
                    for i in range(6)
                ]
                up_split[:used, at] = split_three(jnp.concatenate(both[:3], axis=0))
                lo_split[:used, at] = split_three(jnp.concatenate(both[3:], axis=0))

        upper = up_split
        lower = up_split if single else lo_split

        def lowered(y):
            return pltpu.roll(y, 8 - DIM, 0) if single else y

        @pl.loop(0, halo // halo_chunk)
        def _(c):
            at = pl.ds(pl.multiple_of(poses + c * halo_chunk, halo_chunk), halo_chunk)
            stage_field(lowered(fold(dot_nt(lower[:used, :], dst_hot[at, :]), rows)), rows, c)

        post(ex + 1, tiles, [])

        @pl.loop(0, poses // CHUNK)
        def _(c):
            at = chunk_of(c)
            result[:rows, at] = fold(dot_nt(upper[:used, :], src_hot[at, :]), rows) + lowered(
                fold(dot_nt(lower[:used, :], dst_hot[at, :]), rows)
            )

        arrive(ex + 1, tiles)
        h_split[:used, :] = split_three(unpack(ex + 1, tiles))

        @pl.loop(0, poses // CHUNK)
        def _(c):
            at = chunk_of(c)
            result[:rows, at] += fold(dot_nt(h_split[:used, :], send_hot[at, :]), rows)

        return result[:rows, :], arrived_scalars(ex, len(scalars))

    def summed(ex, scalars):
        post(ex, 0, scalars)
        arrive(ex, 0)
        return arrived_scalars(ex, len(scalars))

    hot(send_hot, send_index[...], poses)

    frame_now = []
    padding = jnp.zeros((8 - RANK, poses), F32)
    for d in range(DIM):
        rows = [frames[3 * a + d:3 * a + d + 1, :] for a in range(RANK)]
        frame_now.append(jnp.concatenate(rows + [padding], axis=0))
    vector = [start[d:d + 1, :] for d in range(DIM)]
    copy_row = lax.broadcasted_iota(jnp.int32, (8, poses), 0)

    def build():
        hot(src_hot, source[...], poses)
        hot(dst_hot, target[...], poses + halo)
        live = lax.broadcasted_iota(jnp.int32, (1, edges), 1) < count[...]
        weight = jnp.where(live, 0.5, 0.0)
        for j in range(6):
            for i in range(6):
                a, b = 6 * i + j, 6 * j + i
                coupling[8 * j + i:8 * j + i + 1, :] = weight * (
                    blocks[a:a + 1, :] + blocks[b:b + 1, :]
                )
            coupling[8 * j + 6:8 * j + 8, :] = jnp.zeros((2, edges), F32)

    def stacked(parts):
        return jnp.concatenate(parts, axis=0)

    square = sum(total(v * v) for v in vector)
    joint = stacked([jnp.where(copy_row == RANK, vector[d], frame_now[d]) for d in range(DIM)])
    image, (start_square,) = product(joint, DIM, 0, [square], before=build)
    euclidean = [image[8 * d:8 * d + 8] for d in range(DIM)]
    start_scale = 1.0 / jnp.sqrt(start_square / entries + epsilon)
    start_image = [euclidean[d][RANK:RANK + 1] * start_scale for d in range(DIM)]
    krylov = [[v * start_scale for v in vector]]

    projected = right_product(frame_now, multiplier(frame_now, euclidean))
    gradient = [
        jnp.where(copy_row < RANK, 2.0 * (euclidean[d] - projected[d]), 0.0) for d in range(DIM)
    ]
    (square,) = summed(2, [sum(total(g * g) for g in gradient)])
    length = step_length * (float(poses * shards) ** 0.5) / jnp.sqrt(square + epsilon)
    moved = [frame_now[d] - length * gradient[d] for d in range(DIM)]
    norms = column_sum(sum(m * m for m in moved))
    scale = jnp.sqrt(DIM / norms)
    polar = [m * scale for m in moved]
    for _ in range(polar_steps):
        gram = [[None] * DIM for _ in range(DIM)]
        for d in range(DIM):
            for e in range(d, DIM):
                value = -0.5 * column_sum(polar[d] * polar[e])
                gram[d][e] = gram[e][d] = value + 1.5 if d == e else value
        polar = right_product(polar, gram)
    for d in range(DIM):
        for a in range(RANK):
            new_frames[3 * a + d:3 * a + d + 1, :] = polar[d][a:a + 1]

    image, _ = product(stacked(polar), DIM, 3, [])
    certificate = multiplier(polar, [image[8 * d:8 * d + 8] for d in range(DIM)])

    def certify(image_rows, vec):
        back = right_product(vec, certificate)
        return [image_rows[d] - back[d] for d in range(DIM)]

    images = [certify(start_image, krylov[0])]
    alphas, betas = [], []
    for k in range(LANCZOS):
        current = images[-1]
        dots = [
            total(sum(member[d] * current[d] for d in range(DIM))) for member in krylov
        ] + [total(sum(c * c for c in current))]
        ex = 5 + 2 * k
        if k < LANCZOS - 1:
            rows = stacked(current + [jnp.zeros((8 - DIM, poses), F32)])
            image, sums = product(rows, 1, ex, dots)
            following = certify([image[d:d + 1] for d in range(DIM)], current)
        else:
            sums = summed(ex, dots)
        weights = [s / entries for s in sums[:-1]]
        beta = jnp.sqrt(sums[-1] / entries - sum(h * h for h in weights) + epsilon)
        inverse = 1.0 / beta
        krylov.append([
            (current[d] - sum(h * q[d] for h, q in zip(weights, krylov))) * inverse
            for d in range(DIM)
        ])
        if k < LANCZOS - 1:
            images.append([
                (following[d] - sum(h * w[d] for h, w in zip(weights, images))) * inverse
                for d in range(DIM)
            ])
        alphas.append(weights[-1])
        betas.append(beta)
    for d in range(DIM):
        last_vector[d:d + 1, :] = krylov[-1][d]
    column = lax.broadcasted_iota(jnp.int32, (2, LANCZOS), 1)
    line = lax.broadcasted_iota(jnp.int32, (2, LANCZOS), 0)
    table = jnp.zeros((2, LANCZOS), F32)
    for k in range(LANCZOS):
        table = jnp.where(column == k, jnp.where(line == 0, alphas[k], betas[k]), table)
    tridiagonal[...] = table

    tiles_of = [DIM, DIM, 0, DIM, DIM] + [1] * (2 * (LANCZOS - 1)) + [0]
    for ex in range(EXCHANGES):
        rows = ROWS[tiles_of[ex]]
        whole = send.at[ex, pl.ds(0, shards - 1), pl.ds(0, rows)]
        pltpu.make_async_copy(whole, whole, send_sem.at[ex]).wait()


def on_device(shards, sub_size, frames, start, blocks, source, target, count, send_index):
    poses = frames.shape[1]
    edges = source.shape[1]
    halo = send_index.shape[1]
    vmem = pl.BlockSpec(memory_space=pltpu.VMEM)
    split_rows = 3 * 8 * DIM + 8
    return pl.pallas_call(
        functools.partial(kernel, shards, sub_size),
        out_shape=(
            jax.ShapeDtypeStruct((RANK * DIM, poses), F32),
            jax.ShapeDtypeStruct((DIM, poses), F32),
            jax.ShapeDtypeStruct((2, LANCZOS), F32),
        ),
        in_specs=[vmem] * 7,
        out_specs=(vmem, vmem, vmem),
        scratch_shapes=[
            pltpu.VMEM((poses, edges), F8),
            pltpu.VMEM((poses + halo, edges), F8),
            pltpu.VMEM((poses, halo), F8),
            pltpu.VMEM((48, edges), F32),
            pltpu.VMEM((8 * DIM, edges), F32),
            pltpu.VMEM((8 * DIM, edges), F32),
            pltpu.VMEM((split_rows, poses), BF16),
            pltpu.VMEM((split_rows, halo), BF16),
            pltpu.VMEM((split_rows, edges), BF16),
            pltpu.VMEM((split_rows, edges), BF16),
            pltpu.VMEM((halo // LANES, 8 * DIM, LANES), F32),
            pltpu.VMEM((8 * DIM, poses), F32),
            pltpu.VMEM((EXCHANGES, shards, 8, LANES), F32),
            pltpu.VMEM((EXCHANGES, shards, 8, LANES), F32),
            pltpu.SemaphoreType.DMA((EXCHANGES,)),
            pltpu.SemaphoreType.DMA((EXCHANGES,)),
        ],
        compiler_params=pltpu.CompilerParams(
            collective_id=0, has_side_effects=True, vmem_limit_bytes=60 * 1024 * 1024
        ),
    )(frames, start, blocks, source, target, count.reshape(1, 1), send_index)


def solution(mesh):
    shards = mesh.shape["rows"] * mesh.shape["sub"]
    in_specs = (
        P(None, ("rows", "sub")),
        P(None, ("rows", "sub")),
        P(None, ("rows", "sub")),
        P(("rows", "sub"), None),
        P(("rows", "sub"), None),
        P(("rows", "sub")),
        P(("rows", "sub"), None),
    )
    out_specs = (P(None, ("rows", "sub")), P(None, ("rows", "sub")), P())
    return jax.shard_map(
        functools.partial(on_device, shards, mesh.shape["sub"]),
        mesh=mesh,
        in_specs=in_specs,
        out_specs=out_specs,
        check_vma=False,
    )
```
